32 devices in a mesh: pts: 16 (over z, x, core), bond: 2 (over y).
Axes of the slice: x: 2, y: 2, z: 4, core: 2. Of those that a mesh axis runs over, the one named last changes fastest.
Arguments:
- displacement: float32 [3, 64, 64, 256], P(None, 'pts', 'bond'), may hold values from -1.5 to 1.5
- velocity: float32 [3, 64, 64, 256], P(None, 'pts', 'bond'), may hold values from -6 to 6
- stiffness: float32 [64, 64, 256], P('pts', 'bond'), may hold values from 0.5 to 8
- offsets: int32 [256, 3], P('bond'), may hold values from -4 to 4, as said below
- intact: int32 [256, 64, 64, 256], P('bond', 'pts'), may hold values 0 or 1
Outputs:
- new_displacement: float32 [3, 64, 64, 256], P(None, 'pts', 'bond')
- new_velocity: float32 [3, 64, 64, 256], P(None, 'pts', 'bond')
The draws below stay inside these ranges and needn't reach their ends.
Inputs may be any that keep to these rules, and one draw needn't show every extreme that they name: `offsets`: every nonzero lattice shift (a, b, c) with a * a + b * b + c * c <= 16, each exactly once, in an order drawn from the seed.
All inputs are finite; a program needn't handle non-finite values. No bound on the sum of `intact` on one device may be relied on, other than what follows from the above.
Results may differ from the reference program's by a relative error of at most 0.0003.
Values sent between devices are 32-bit elements; how exact they have to be, the bound alone decides.
No kernel may reach another device: no remote copies, remote signals or barrier semaphores. Data moves between devices by JAX's collectives and lax.ppermute only.
A program may use at most 128 MiB of HBM per device.

```python
import math
import jax
import jax.numpy as jnp
from jax import lax

REACH = 4
OFFSETS = 256
NY = 64
NZ = 256
NX = 64


def draw_offsets(key, part):
    side = 2 * REACH + 1
    shuffled = jax.random.permutation(key, side * side * side).astype(jnp.int32)
    first = shuffled // (side * side) - REACH
    second = shuffled // side % side - REACH
    third = shuffled % side - REACH
    radius = first * first + second * second + third * third
    outside = ((radius > REACH * REACH) | (radius == 0)).astype(jnp.int32)
    order = jnp.argsort(outside, stable=True)[:OFFSETS]
    return jnp.stack([first[order], second[order], third[order]], axis=1).astype(jnp.int32)


def touch_ends(entries, own_key, smallest, top_value):
    longest = entries.shape.index(max(entries.shape))
    spots = []
    for shift in (0, 1):
        where = [jax.random.randint(jax.random.fold_in(own_key, axis), (), 0, length) for axis, length in enumerate(entries.shape)]
        where[longest] = (where[longest] + shift) % entries.shape[longest]
        spots.append(tuple(where))
    return entries.at[spots[0]].set(smallest).at[spots[1]].set(top_value)


def level_of(key, shape, cuts, smallest, largest):
    factor_of, own = 1.0, jax.random.fold_in(key, 6)
    for axis_at, shards_of in cuts:
        heights = jnp.exp(jax.random.uniform(jax.random.fold_in(own, axis_at), (shards_of,), jnp.float32, smallest / len(cuts), largest / len(cuts)))
        factor_of = factor_of * jnp.repeat(heights, shape[axis_at] // shards_of).reshape([-1 if axis == axis_at else 1 for axis in range(len(shape))])
    return factor_of


def centred(own_key, extent, deviation, bound, cuts=(), kind=jnp.bfloat16):
    values = jax.random.normal(own_key, extent, jnp.float32) * deviation
    if len(cuts) > 0:
        values = level_of(own_key, extent, cuts, -0.22, 0.18) * values
    return jnp.clip(values, min=-bound, max=bound).astype(kind)


def setup_inputs(seed: int = 0) -> dict:
    splits = jax.random.split(jax.random.key(seed), 6)
    return {
        "displacement": centred(splits[0], (3, NX, NY, NZ), 0.5, 1.5, ((1, 16), (2, 2)), jnp.float32),
        "velocity": centred(splits[1], (3, NX, NY, NZ), 1.0, 6.0, ((1, 16), (2, 2)), jnp.float32),
        "stiffness": jnp.clip(jnp.exp(math.log(8.0) - 2.7725887 * jax.random.uniform(splits[2], (NX, NY, NZ), jnp.float32) ** level_of(splits[2], (NX, NY, NZ), ((0, 16), (1, 2)), -0.2, 0.2)), 0.5, 8.0),
        "offsets": draw_offsets(jax.random.fold_in(splits[5], 71), 0),
        "intact": touch_ends((jax.random.randint(splits[4], (OFFSETS, NX, NY, NZ), 0, 4) < 3).astype(jnp.int32), jax.random.fold_in(splits[4], 1), 0, 1),
    }


SPACING = 6.0
FORCE_SCALE = 8.0
TIME_STEP = 0.5

def bond_forces(centre, padded, inside, shift, alive):
    shape = centre.shape
    lower = (shift + REACH).astype(jnp.int32)
    anchor = jnp.zeros((), jnp.int32)
    nearby = lax.dynamic_slice(padded, (anchor, lower[0], lower[1], lower[2]), shape)
    present = lax.dynamic_slice(inside, (lower[0], lower[1], lower[2]), shape[1:]) * alive.astype(centre.dtype)
    bond_vec = shift.astype(centre.dtype) * SPACING
    length = jnp.sqrt(jnp.sum(bond_vec * bond_vec))
    relative = bond_vec[:, None, None, None] + nearby[:3] - centre[:3]
    stretched = jnp.sqrt(lax.optimization_barrier(jnp.sum(relative * relative, axis=0)))
    strain = (stretched - length) / length
    coupling = 0.5 * (centre[3] + nearby[3]) * present / length
    return relative * (coupling * strain / stretched)

def reference(displacement, velocity, stiffness, offsets, intact):
    centre = jnp.concatenate([displacement, stiffness[None]], axis=0)
    padded = jnp.pad(centre, ((0, 0), (REACH, REACH), (REACH, REACH), (REACH, REACH)))
    inside = jnp.pad(jnp.ones(stiffness.shape, jnp.float32), REACH)

    def accumulate(total, pieces):
        shift, alive = pieces
        return (total + bond_forces(centre, padded, inside, shift, alive), None)
    total = lax.scan(accumulate, jnp.zeros(displacement.shape, jnp.float32), (offsets, intact))[0]
    density = FORCE_SCALE * total
    new_velocity = velocity + TIME_STEP * density
    new_displacement = displacement + TIME_STEP * new_velocity
    return (new_displacement, new_velocity)
```

```python
import functools
import math

import jax
import jax.numpy as jnp
from jax import lax
from jax.experimental import pallas as pl
from jax.experimental.pallas import tpu as pltpu
from jax.sharding import PartitionSpec as P

REACH = 4
SPACING = 6.0
FORCE_SCALE = 8.0
TIME_STEP = 0.5
LANES = 128
TILE = 8
BLOCK_ROWS = 16
UNROLL = 4


def plane_reach(c):
    return math.isqrt(REACH * REACH - c * c)


def copy_bases(slab):
    bases, total = [], 0
    for c in range(-REACH, REACH + 1):
        bases.append(total + plane_reach(c))
        total += slab + 2 * plane_reach(c)
    return bases, total


def build_tables(state, copies, outside, px, py, slab, rows, halves):
    stride = rows + TILE
    bases, total = copy_bases(slab)
    zero = jnp.zeros((TILE, LANES), jnp.float32)
    lane = lax.broadcasted_iota(jnp.int32, (TILE, LANES), 1)
    row = lax.broadcasted_iota(jnp.int32, (TILE, LANES), 0)

    def clear(n, carry):
        copies[pl.ds(pl.multiple_of(n * stride, TILE), TILE), :] = zero
        return carry

    lax.fori_loop(0, total * 4 * halves + 1, clear, 0, unroll=4)
    for c in range(-REACH, REACH + 1):
        reach = plane_reach(c)

        def one_plane(t, carry, c=c, reach=reach):
            source = t + REACH - reach
            first = (bases[c + REACH] - reach + t) * (4 * halves)
            for field in range(4):
                for tile in range(rows // TILE):
                    parts = [
                        state[field, source, tile * TILE : (tile + 1) * TILE, h * LANES : (h + 1) * LANES]
                        for h in range(halves)
                    ]
                    if field == 2 and c != 0:
                        parts = [part + SPACING * c for part in parts]
                    if c != 0:
                        turned = [pltpu.roll(part, (-c) % LANES, 1) for part in parts]
                        parts = []
                        for h in range(halves):
                            if c > 0:
                                other = turned[h + 1] if h + 1 < halves else None
                                keep = lane < LANES - c
                            else:
                                other = turned[h - 1] if h > 0 else None
                                keep = lane >= -c
                            parts.append(turned[h] if other is None else jnp.where(keep, turned[h], other))
                    for h in range(halves):
                        at = (first + field * halves + h) * stride + TILE + tile * TILE
                        copies[pl.ds(pl.multiple_of(at, TILE), TILE), :] = parts[h]
            return carry

        lax.fori_loop(0, slab + 2 * reach, one_plane, 0)
        for h in range(halves):
            z = lane + (h * LANES + c)
            z_out = (z < 0) | (z >= halves * LANES)
            for tile in range(-1, rows // TILE + 1):
                r = row + tile * TILE
                out = z_out | (r < 0) | (r >= rows)
                at = ((c + REACH) * halves + h) * (rows + 2 * TILE) + (tile + 1) * TILE
                outside[at : at + TILE, :] = out.astype(jnp.int32)

    def one_tile(n, carry):
        tiles = rows // TILE
        plane = n // (halves * tiles)
        tile = n % tiles
        at = pl.multiple_of(tile * TILE, TILE)
        for h in range(halves):
            ux = state[0, REACH + plane, pl.ds(at, TILE), h * LANES : (h + 1) * LANES]
            uy = state[1, REACH + plane, pl.ds(at, TILE), h * LANES : (h + 1) * LANES]
            for s in range(2 * REACH + 1):
                to = ((s * slab + plane) * halves + h) * rows + tile * TILE
                px[pl.ds(pl.multiple_of(to, TILE), TILE), :] = ux - SPACING * (s - REACH)
                py[pl.ds(pl.multiple_of(to, TILE), TILE), :] = uy - SPACING * (s - REACH)
        return carry

    def plane_tiles(n, carry):
        tiles = rows // TILE
        return one_tile((n // tiles) * (halves * tiles) + n % tiles, carry)

    lax.fori_loop(0, slab * (rows // TILE), plane_tiles, 0)


def force_kernel(index, invlen, coef, state, mask, out, copies, outside, px, py, *, slab, rows, halves, count, unroll):
    i = pl.program_id(0)
    block = pl.program_id(1)

    @pl.when((i == 0) & (block == 0))
    def _():
        build_tables(state, copies, outside, px, py, slab, rows, halves)

    stride = rows + TILE
    block_rows = mask.shape[2]
    units = [(tile, h) for tile in range(block_rows // TILE) for h in range(halves)]
    row0 = block * block_rows
    own = {}
    for tile, h in units:
        at = pl.multiple_of(row0 + tile * TILE, TILE)
        own[tile, h] = [
            state[f, REACH + i, pl.ds(at, TILE), h * LANES : (h + 1) * LANES] for f in (2, 3)
        ]
    plane_step = i * (4 * halves * stride) + row0
    own_step = i * (halves * rows) + row0

    def step(g, totals):
        totals = list(totals)
        for u in range(unroll):
            k = g * unroll + u
            q = index[0, k] + plane_step
            o = index[1, k] + row0
            ax = index[2, k] + own_step
            ay = index[3, k] + own_step
            inverse = invlen[k]
            weight = coef[i, k]
            for n, (tile, h) in enumerate(units):
                def near(field):
                    return copies[pl.ds(q + ((field * halves + h) * stride + tile * TILE), TILE), :]

                pz, kp = own[tile, h]
                rx = near(0) - px[pl.ds(pl.multiple_of(ax + (h * rows + tile * TILE), TILE), TILE), :]
                ry = near(1) - py[pl.ds(pl.multiple_of(ay + (h * rows + tile * TILE), TILE), TILE), :]
                rz = near(2) - pz
                inv = lax.rsqrt(rx * rx + ry * ry + rz * rz)
                gone = outside[pl.ds(o + (h * (rows + 2 * TILE) + tile * TILE), TILE), :]
                alive = mask[k, 0, tile * TILE : (tile + 1) * TILE, h * LANES : (h + 1) * LANES]
                factor = jnp.where(alive > gone, weight, 0.0)
                w = (inverse - inv) * (near(3) + kp) * factor
                totals[3 * n] += w * rx
                totals[3 * n + 1] += w * ry
                totals[3 * n + 2] += w * rz
        return tuple(totals)

    zero = jnp.zeros((TILE, LANES), jnp.float32)
    totals = lax.fori_loop(0, count // unroll, step, (zero,) * (3 * len(units)))
    for n, (tile, h) in enumerate(units):
        for f in range(3):
            out[f, 0, tile * TILE : (tile + 1) * TILE, h * LANES : (h + 1) * LANES] = totals[3 * n + f]


def bond_tables(offsets, slab, rows, halves):
    stride = rows + TILE
    bases, _ = copy_bases(slab)
    shift = offsets.astype(jnp.int32)
    a, b, c = shift[:, 0], shift[:, 1], shift[:, 2]
    base = jnp.zeros_like(c)
    for s in range(-REACH, REACH + 1):
        base = jnp.where(c == s, bases[s + REACH], base)
    index = jnp.stack(
        [
            (base + a) * (4 * halves * stride) + TILE + b,
            (c + REACH) * (halves * (rows + 2 * TILE)) + TILE + b,
            (a + REACH) * (slab * halves * rows),
            (b + REACH) * (slab * halves * rows),
        ]
    )
    inverse = 1.0 / (SPACING * jnp.sqrt((a * a + b * b + c * c).astype(jnp.float32)))
    plane = lax.axis_index("pts") * slab + jnp.arange(slab, dtype=jnp.int32)[:, None] + a[None]
    valid = (plane >= 0) & (plane < slab * lax.axis_size("pts"))
    coef = jnp.where(valid, 0.5 * FORCE_SCALE * TIME_STEP * inverse[None], 0.0)
    return index, inverse, coef


def forces(index, inverse, coef, state, intact):
    _, padded, rows, width = state.shape
    slab, count = intact.shape[1], intact.shape[0]
    halves = width // LANES
    _, total = copy_bases(slab)
    block_rows = math.gcd(rows, BLOCK_ROWS)
    unroll = math.gcd(count, UNROLL)
    body = functools.partial(
        force_kernel, slab=slab, rows=rows, halves=halves, count=count, unroll=unroll
    )
    smem = pl.BlockSpec(memory_space=pltpu.SMEM)
    return pl.pallas_call(
        body,
        out_shape=jax.ShapeDtypeStruct((3, slab, rows, width), jnp.float32),
        grid=(slab, rows // block_rows),
        in_specs=[
            smem,
            smem,
            smem,
            pl.BlockSpec(state.shape, lambda i, j: (0, 0, 0, 0), pipeline_mode=pl.Buffered(1)),
            pl.BlockSpec((count, 1, block_rows, width), lambda i, j: (0, i, j, 0)),
        ],
        out_specs=pl.BlockSpec((3, 1, block_rows, width), lambda i, j: (0, i, j, 0)),
        scratch_shapes=[
            pltpu.VMEM((total * 4 * halves * (rows + TILE) + TILE, LANES), jnp.float32),
            pltpu.VMEM(((2 * REACH + 1) * halves * (rows + 2 * TILE), LANES), jnp.int32),
            pltpu.VMEM(((2 * REACH + 1) * slab * halves * rows, LANES), jnp.float32),
            pltpu.VMEM(((2 * REACH + 1) * slab * halves * rows, LANES), jnp.float32),
        ],
        compiler_params=pltpu.CompilerParams(
            dimension_semantics=("arbitrary", "arbitrary"), vmem_limit_bytes=62 * 1024 * 1024
        ),
        name="bonds",
    )(index, inverse, coef, state, intact)


def gather_rows(block, axis, dim):
    count = lax.axis_size(axis)
    me = lax.axis_index(axis)
    width = block.shape[dim]
    shape = list(block.shape)
    shape[dim] = width * count
    whole = lax.dynamic_update_slice_in_dim(jnp.zeros(shape, block.dtype), block, me * width, dim)
    for s in range(1, count):
        other = lax.ppermute(block, axis, [(j, (j + s) % count) for j in range(count)])
        whole = lax.dynamic_update_slice_in_dim(whole, other, (me - s) % count * width, dim)
    return whole


def scatter_rows(block, axis, dim):
    count = lax.axis_size(axis)
    me = lax.axis_index(axis)
    width = block.shape[dim] // count
    total = lax.dynamic_slice_in_dim(block, me * width, width, dim)
    for s in range(1, count):
        part = lax.dynamic_slice_in_dim(block, (me + s) % count * width, width, dim)
        total = total + lax.ppermute(part, axis, [(j, (j + s) % count) for j in range(count)])
    return total


def on_device(displacement, velocity, stiffness, offsets, intact):
    slab = displacement.shape[1]
    own = jnp.concatenate([displacement, stiffness[None]], axis=0)
    whole = gather_rows(own, "bond", 2)
    count = lax.axis_size("pts")
    forward = [(i, i + 1) for i in range(count - 1)]
    low = lax.ppermute(whole[:, slab - REACH :], "pts", forward)
    high = lax.ppermute(whole[:, :REACH], "pts", [(t, s) for s, t in forward])
    state = jnp.concatenate([low, whole, high], axis=1)
    index, inverse, coef = bond_tables(offsets, slab, state.shape[2], state.shape[3] // LANES)
    partial = forces(index, inverse, coef, state, intact)
    new_velocity = velocity + scatter_rows(partial, "bond", 2)
    new_displacement = displacement + TIME_STEP * new_velocity
    return (new_displacement, new_velocity)


def solution(mesh):
    return jax.shard_map(
        on_device,
        mesh=mesh,
        in_specs=(
            P(None, "pts", "bond", None),
            P(None, "pts", "bond", None),
            P("pts", "bond", None),
            P("bond", None),
            P("bond", "pts", None, None),
        ),
        out_specs=(P(None, "pts", "bond", None), P(None, "pts", "bond", None)),
        check_vma=False,
    )
```

```python
import functools
import math

import jax
import jax.numpy as jnp
from jax import lax
from jax.experimental import pallas as pl
from jax.experimental.pallas import tpu as pltpu
from jax.sharding import PartitionSpec as P

REACH = 4
SPACING = 6.0
FORCE_SCALE = 8.0
TIME_STEP = 0.5
LANES = 128
TILE = 8
LONG = 16
SHORT = 4
SLOTS = 3
PARTS = 8
SHIFTS = 2 * REACH + 1


def cut(d):
    return math.isqrt(REACH * REACH - d * d)


def copy_bases(slab, halo):
    low, high, total = [], [], 0
    for c in range(-REACH, REACH + 1):
        if halo:
            low.append(total + cut(c))
            high.append(total + cut(c) - slab)
            total += 2 * cut(c)
        else:
            low.append(total)
            high.append(total)
            total += slab
    return low, high, total


ROWS_OF_LIST = 8


def lists_kernel(device, shift, lists, inverses, *, slab, rows, halves, slabs, halo):
    stride = rows + TILE
    low, high, _ = copy_bases(slab, halo)
    a, b, c = [shift[n : n + 1, :] for n in range(3)]
    count = shift.shape[1]
    first = device[0] * slab
    inverse = 1.0 / (SPACING * jnp.sqrt((a * a + b * b + c * c).astype(jnp.float32)))
    bond = lax.broadcasted_iota(jnp.int32, (1, count), 1)
    down = lax.broadcasted_iota(jnp.int32, (count, count), 0)
    across = lax.broadcasted_iota(jnp.int32, (count, count), 1)
    earlier = (down < across).astype(jnp.float32)
    for i in range(slab):
        plane = a + i
        inside = (plane >= 0) & (plane < slab)
        if halo:
            whole = plane + first
            member = (~inside) & (whole >= 0) & (whole < slab * slabs)
        else:
            member = inside
        base = jnp.zeros_like(plane)
        for n in range(SHIFTS):
            base = jnp.where(c == n - REACH, jnp.where(plane < 0, low[n], high[n]), base)
        ones = jnp.where(member, 1.0, 0.0)
        place = jnp.dot(jnp.broadcast_to(ones, (8, count)), earlier, precision=lax.Precision.HIGHEST)[0:1]
        spot = (place.astype(jnp.int32) == down) & (jnp.broadcast_to(ones, (count, count)) > 0.5)
        values = [
            (base + plane) * (4 * halves * stride) + TILE + b,
            (c + REACH) * (halves * (rows + 2 * TILE)) + TILE + b,
            ((b + REACH) * slab + i) * (halves * rows),
            bond,
        ]
        values = [v.astype(jnp.float32) for v in values] + [inverse] + [jnp.zeros_like(inverse)] * 3
        table = lax.dot_general(
            jnp.concatenate(values, axis=0),
            jnp.where(spot, 1.0, 0.0),
            (((1,), (1,)), ((), ())),
            precision=lax.Precision.HIGHEST,
            preferred_element_type=jnp.float32,
        )
        number = jnp.broadcast_to(jnp.sum(ones, axis=1, keepdims=True), (1, count))
        at = i * ROWS_OF_LIST
        lists[at : at + 4, :] = (table[0:4] + 0.5).astype(jnp.int32)
        lists[at + 4 : at + 5, :] = number.astype(jnp.int32)
        lists[at + 5 : at + 8, :] = jnp.zeros((3, count), jnp.int32)
        inverses[i : i + 1, :] = table[4:5]


def bond_lists(offsets, slab, rows, halves, halo):
    count = offsets.shape[0]
    body = functools.partial(
        lists_kernel, slab=slab, rows=rows, halves=halves, slabs=lax.axis_size("pts"), halo=halo
    )
    device = lax.axis_index("pts").astype(jnp.int32).reshape(1)
    vmem = pl.BlockSpec(memory_space=pltpu.VMEM)
    lists, inverses = pl.pallas_call(
        body,
        out_shape=(
            jax.ShapeDtypeStruct((slab * ROWS_OF_LIST, count), jnp.int32),
            jax.ShapeDtypeStruct((slab, count), jnp.float32),
        ),
        in_specs=[pl.BlockSpec(memory_space=pltpu.SMEM), vmem],
        out_specs=(vmem, vmem),
        cost_estimate=pl.CostEstimate(flops=8_000_000, transcendentals=0, bytes_accessed=0),
        name="halo_lists" if halo else "own_lists",
    )(device, offsets.astype(jnp.int32).T)
    return lists.reshape(-1), inverses.reshape(-1)


def shifted(parts, c, lane):
    if c == 0:
        return parts
    turned = [pltpu.roll(part, (-c) % LANES, 1) for part in parts]
    result = []
    for h in range(len(parts)):
        other = h + 1 if c > 0 else h - 1
        if 0 <= other < len(parts):
            keep = lane < LANES - c if c > 0 else lane >= -c
            result.append(jnp.where(keep, turned[h], turned[other]))
        else:
            result.append(turned[h])
    return result


def bonds_kernel(lists, inverses, places, *refs, halo, slab, rows, halves, count, pieces, segments, seg_rows, started, started_at):
    refs = list(refs)
    take = lambda n: [refs.pop(0) for _ in range(n)]
    own = take(pieces)
    lows = take(pieces) if halo else []
    highs = take(pieces) if halo else []
    mask = refs.pop(0)
    init = refs.pop(0) if started else None
    out, copies, outside, py, plain, buffer, sems = refs
    stride = rows + TILE
    width = own[0].shape[2]
    tiles = width // TILE
    low, high, total = copy_bases(slab, halo)
    middle = 0.5 * (slab - 1)
    lane = lax.broadcasted_iota(jnp.int32, (TILE, LANES), 1)
    row = lax.broadcasted_iota(jnp.int32, (TILE, LANES), 0)
    zero = jnp.zeros((TILE, LANES), jnp.float32)
    me = places[0]

    def first_row(s):
        if s == 0:
            return pl.multiple_of(me * width, TILE)
        below = me - s
        return pl.multiple_of(jnp.where(below < 0, below + pieces, below) * width, TILE)

    piece_row = [first_row(s) for s in range(pieces)]
    parts = sems.shape[1]
    each = count // parts
    items = len(segments) * slab

    def seg_row(g):
        row0 = piece_row[segments[0]]
        for n, s in enumerate(segments):
            row0 = jnp.where(g == n, piece_row[s], row0)
        return pl.multiple_of(row0, TILE)

    def fetch(t, slot):
        at = seg_row(t // slab)
        return [
            pltpu.make_async_copy(
                mask.at[pl.ds(n * each, each), t % slab, pl.ds(at, seg_rows), :],
                buffer.at[slot, pl.ds(n * each, each)],
                sems.at[slot, n],
            )
            for n in range(parts)
        ]

    for t in range(min(SLOTS - 1, items)):
        for copy in fetch(t, t):
            copy.start()

    def clear(n, carry):
        copies[pl.ds(pl.multiple_of(n * stride, TILE), TILE), :] = zero
        return carry

    lax.fori_loop(0, total * 4 * halves, clear, 0, unroll=16)
    copies[total * 4 * halves * stride : total * 4 * halves * stride + TILE, :] = zero

    def spread(piece, field, plane, x, first_row, places_of):
        along_x = jnp.where(field == 0, x, 0.0)
        along_z = jnp.where(field == 2, SPACING, 0.0)
        for tile in range(tiles):
            at = tile * TILE
            parts = [
                piece[field, plane, at : at + TILE, h * LANES : (h + 1) * LANES] + along_x
                for h in range(halves)
            ]
            for c, to in places_of:
                moved = shifted([part + along_z * float(c) if c else part for part in parts], c, lane)
                for h in range(halves):
                    put = (to * 4 + field) * (halves * stride) + (h * stride + TILE + at)
                    copies[pl.ds(pl.multiple_of(first_row + put, TILE), TILE), :] = moved[h]

    def one_field(field, carry):
        for s in range(pieces):
            if halo:
                for d in range(1, REACH + 1):
                    span = range(-cut(d), cut(d) + 1)
                    below = [(c, low[c + REACH] - d) for c in span]
                    above = [(c, high[c + REACH] + slab + d - 1) for c in span]
                    spread(lows[s], field, REACH - d, SPACING * (-d - middle), piece_row[s], below)
                    spread(highs[s], field, d - 1, SPACING * (slab + d - 1 - middle), piece_row[s], above)
            else:
                for i in range(slab):
                    to = [(c, low[c + REACH] + i) for c in range(-REACH, REACH + 1)]
                    spread(own[s], field, i, SPACING * (i - middle), piece_row[s], to)
        return carry

    lax.fori_loop(0, 4, one_field, 0)

    for c in range(-REACH, REACH + 1):
        for h in range(halves):
            z = lane + (h * LANES + c)
            z_out = (z < 0) | (z >= halves * LANES)
            for tile in range(-1, rows // TILE + 1):
                r = row + tile * TILE
                gone = z_out | (r < 0) | (r >= rows)
                at = ((c + REACH) * halves + h) * (rows + 2 * TILE) + (tile + 1) * TILE
                outside[at : at + TILE, :] = gone.astype(jnp.int32)

    for g, s in enumerate(segments):

        def one_tile(n, carry, s=s, g=g):
            plane = n // (seg_rows // TILE)
            at = n % (seg_rows // TILE) * TILE
            source = pl.ds(pl.multiple_of(at, TILE), TILE)
            x = SPACING * (plane.astype(jnp.float32) - middle)
            for h in range(halves):
                lanes = slice(h * LANES, (h + 1) * LANES)
                to = (plane * halves + h) * rows + g * seg_rows + at
                here = pl.ds(pl.multiple_of(to, TILE), TILE)
                plain[0, here, :] = own[s][0, plane, source, lanes] + x
                plain[1, here, :] = own[s][2, plane, source, lanes]
                plain[2, here, :] = own[s][3, plane, source, lanes]
                uy = own[s][1, plane, source, lanes]
                for n in range(SHIFTS):
                    there = pl.ds(pl.multiple_of(to + n * (slab * halves * rows), TILE), TILE)
                    py[there, :] = uy - SPACING * (n - REACH)
            return carry

        lax.fori_loop(0, slab * (seg_rows // TILE), one_tile, 0, unroll=2)

    short = math.gcd(count, SHORT)

    def one_item(t, carry):
        slot = lax.rem(t, SLOTS)
        for copy in fetch(t, slot):
            copy.wait()

        @pl.when(t + SLOTS - 1 < items)
        def _():
            for copy in fetch(t + SLOTS - 1, lax.rem(t + SLOTS - 1, SLOTS)):
                copy.start()

        g, i = t // slab, t % slab
        row0 = seg_row(g)
        table = i * (ROWS_OF_LIST * count)
        bonds = lists[table + 4 * count]
        whole = bonds // LONG

        def one_unit(n, carry):
            local = g * seg_rows + n * TILE
            here = row0 + n * TILE
            at_p = [pl.multiple_of((i * halves + h) * rows + local, TILE) for h in range(halves)]
            own_x, own_z, own_k = [[plain[f, pl.ds(at_p[h], TILE), :] for h in range(halves)] for f in range(3)]
            mask_row = pl.multiple_of(n * TILE, TILE)

            def step(first, number, totals):
                totals = list(totals)
                for u in range(number):
                    e = table + first + u
                    q = lists[e] + here
                    o = lists[e + count] + here
                    ay = lists[e + 2 * count] + local
                    k = lists[e + 3 * count]
                    inverse = inverses[i * count + first + u]
                    for h in range(halves):

                        def near(field):
                            return copies[pl.ds(q + (field * halves + h) * stride, TILE), :]

                        rx = near(0) - own_x[h]
                        ry = near(1) - py[pl.ds(pl.multiple_of(ay + h * rows, TILE), TILE), :]
                        rz = near(2) - own_z[h]
                        inv = lax.rsqrt(rx * rx + ry * ry + rz * rz)
                        gone = outside[pl.ds(o + h * (rows + 2 * TILE), TILE), :]
                        alive = buffer[slot, k, pl.ds(mask_row, TILE), h * LANES : (h + 1) * LANES]
                        factor = jnp.where(alive > gone, inverse, 0.0)
                        w = (inverse - inv) * (near(3) + own_k[h]) * factor
                        totals[3 * h] += w * rx
                        totals[3 * h + 1] += w * ry
                        totals[3 * h + 2] += w * rz
                return tuple(totals)

            totals = (zero,) * (3 * halves)
            totals = lax.fori_loop(0, whole, lambda m, x: step(m * LONG, LONG, x), totals)
            rest = (bonds - whole * LONG + short - 1) // short
            totals = lax.fori_loop(
                0, rest, lambda m, x: step(whole * LONG + m * short, short, x), totals
            )
            for h in range(halves):
                lanes = slice(h * LANES, (h + 1) * LANES)
                for f in range(3):
                    value = totals[3 * h + f]
                    if started:
                        value = value + init[g + started_at, f, i, pl.ds(mask_row, TILE), lanes]
                    out[g, f, i, pl.ds(mask_row, TILE), lanes] = value
            return carry

        lax.fori_loop(0, seg_rows // TILE, one_unit, 0)
        return carry

    lax.fori_loop(0, items, one_item, 0)


def bonds(lists, places, pieces, sides, intact, segments, seg_rows, rows, init, started_at, name, share):
    count, slab, _, depth = intact.shape
    halves = depth // LANES
    halo = sides is not None
    _, _, total = copy_bases(slab, halo)
    blocks = list(pieces) + (list(sides[0]) + list(sides[1]) if halo else [])
    vmem, smem = pl.BlockSpec(memory_space=pltpu.VMEM), pl.BlockSpec(memory_space=pltpu.SMEM)
    started = init is not None
    body = functools.partial(
        bonds_kernel,
        halo=halo,
        slab=slab,
        rows=rows,
        halves=halves,
        count=count,
        pieces=len(pieces),
        segments=segments,
        seg_rows=seg_rows,
        started=started,
        started_at=started_at,
    )
    table = pltpu.VMEM((SHIFTS * slab * halves * rows, LANES), jnp.float32)
    plain = pltpu.VMEM((3, slab * halves * rows, LANES), jnp.float32)
    return pl.pallas_call(
        body,
        out_shape=jax.ShapeDtypeStruct((len(segments), 3, slab, seg_rows, depth), jnp.float32),
        in_specs=[smem] * 3
        + [vmem] * len(blocks)
        + [pl.BlockSpec(memory_space=pl.ANY)]
        + [vmem] * started,
        out_specs=vmem,
        scratch_shapes=[
            pltpu.VMEM((total * 4 * halves * (rows + TILE) + TILE, LANES), jnp.float32),
            pltpu.VMEM((SHIFTS * halves * (rows + 2 * TILE), LANES), jnp.int32),
            table,
            plain,
            pltpu.VMEM((SLOTS, count, seg_rows, depth), jnp.int32),
            pltpu.SemaphoreType.DMA((SLOTS, math.gcd(count, PARTS))),
        ],
        compiler_params=pltpu.CompilerParams(vmem_limit_bytes=60 * 1024 * 1024),
        cost_estimate=pl.CostEstimate(
            flops=int(40 * share * count * slab * rows * depth), transcendentals=0, bytes_accessed=intact.size * 4
        ),
        name=name,
    )(*lists, places, *blocks, intact, *([init] if started else []))


def on_device(displacement, velocity, stiffness, offsets, intact):
    slab, width, depth = stiffness.shape
    rows = intact.shape[2]
    halves = depth // LANES
    number = lax.axis_size("bond")
    me = lax.axis_index("bond")
    count = lax.axis_size("pts")
    forward = [(i, i + 1) for i in range(count - 1)]
    backward = [(t, s) for s, t in forward]

    pieces = [jnp.concatenate([displacement, stiffness[None]], axis=0)]
    for s in range(1, number):
        pieces.append(lax.ppermute(pieces[0], "bond", [(j, (j + s) % number) for j in range(number)]))
    own_lists = bond_lists(offsets, slab, rows, halves, False)
    halo_lists = bond_lists(offsets, slab, rows, halves, True)
    received, own_lists, halo_lists = lax.optimization_barrier((pieces[1:], own_lists, halo_lists))
    pieces = pieces[:1] + list(received)
    lows = [lax.ppermute(x[:, slab - REACH :], "pts", forward) for x in pieces]
    highs = [lax.ppermute(x[:, :REACH], "pts", backward) for x in pieces]
    place = me.astype(jnp.int32).reshape(1)
    every = list(range(number))
    inner = bonds(
        own_lists, place, pieces, None, intact, every, width, rows, None, 0, "own_planes", 0.64
    )
    sides = (lows, highs)
    theirs = bonds(
        halo_lists, place, pieces, sides, intact, every[1:], width, rows, inner, 1,
        "their_rows", 0.36 * (number - 1) / number,
    )
    back = [
        lax.ppermute(theirs[s - 1], "bond", [(j, (j - s) % number) for j in range(number)])
        for s in range(1, number)
    ]
    ours = bonds(
        halo_lists, place, pieces, sides, intact, every[:1], width, rows, inner, 0,
        "our_rows", 0.36 / number,
    )
    total = ours[0]
    for part in back:
        total = total + part
    new_velocity = velocity + (0.5 * FORCE_SCALE * TIME_STEP) * total
    new_displacement = displacement + TIME_STEP * new_velocity
    return (new_displacement, new_velocity)


def solution(mesh):
    return jax.shard_map(
        on_device,
        mesh=mesh,
        in_specs=(
            P(None, "pts", "bond", None),
            P(None, "pts", "bond", None),
            P("pts", "bond", None),
            P("bond", None),
            P("bond", "pts", None, None),
        ),
        out_specs=(P(None, "pts", "bond", None), P(None, "pts", "bond", None)),
        check_vma=False,
    )
```

```python
import functools
import math

import jax
import jax.numpy as jnp
from jax import lax
from jax.experimental import pallas as pl
from jax.experimental.pallas import tpu as pltpu
from jax.sharding import PartitionSpec as P

REACH = 4
SPACING = 6.0
FORCE_SCALE = 8.0
TIME_STEP = 0.5
LANES = 128
TILE = 8
UNIT = 16
LONG = 8
SHORT = 2
SLOTS = 3
PARTS = 8
LIMIT = 28 * 1024 * 1024
SHIFTS = 2 * REACH + 1


def cut(d):
    return math.isqrt(REACH * REACH - d * d)


def copy_bases(slab, halo):
    low, high, total = [], [], 0
    for c in range(-REACH, REACH + 1):
        if halo:
            low.append(total + cut(c))
            high.append(total + cut(c) - slab)
            total += 2 * cut(c)
        else:
            low.append(total)
            high.append(total)
            total += slab
    return low, high, total


ROWS_OF_LIST = 8


def lists_kernel(device, shift, lists, inverses, *, slab, rows, halves, slabs, halo):
    stride = rows + TILE
    low, high, _ = copy_bases(slab, halo)
    a, b, c = [shift[n : n + 1, :] for n in range(3)]
    count = shift.shape[1]
    first = device[0] * slab
    inverse = 1.0 / (SPACING * jnp.sqrt((a * a + b * b + c * c).astype(jnp.float32)))
    bond = lax.broadcasted_iota(jnp.int32, (1, count), 1)
    down = lax.broadcasted_iota(jnp.int32, (count, count), 0)
    across = lax.broadcasted_iota(jnp.int32, (count, count), 1)
    earlier = (down < across).astype(jnp.float32)
    for i in range(slab):
        plane = a + i
        inside = (plane >= 0) & (plane < slab)
        if halo:
            whole = plane + first
            member = (~inside) & (whole >= 0) & (whole < slab * slabs)
        else:
            member = inside
        base = jnp.zeros_like(plane)
        for n in range(SHIFTS):
            base = jnp.where(c == n - REACH, jnp.where(plane < 0, low[n], high[n]), base)
        ones = jnp.where(member, 1.0, 0.0)
        place = jnp.dot(jnp.broadcast_to(ones, (8, count)), earlier, precision=lax.Precision.HIGHEST)[0:1]
        spot = (place.astype(jnp.int32) == down) & (jnp.broadcast_to(ones, (count, count)) > 0.5)
        values = [
            (base + plane) * (4 * halves * stride) + TILE + b,
            (c + REACH) * (halves * (rows + 2 * TILE)) + TILE + b,
            ((b + REACH) * slab + i) * (halves * rows),
            bond,
        ]
        values = [v.astype(jnp.float32) for v in values] + [inverse] + [jnp.zeros_like(inverse)] * 3
        table = lax.dot_general(
            jnp.concatenate(values, axis=0),
            jnp.where(spot, 1.0, 0.0),
            (((1,), (1,)), ((), ())),
            precision=lax.Precision.HIGHEST,
            preferred_element_type=jnp.float32,
        )
        number = jnp.broadcast_to(jnp.sum(ones, axis=1, keepdims=True), (1, count))
        at = i * ROWS_OF_LIST
        lists[at : at + 4, :] = (table[0:4] + 0.5).astype(jnp.int32)
        lists[at + 4 : at + 5, :] = number.astype(jnp.int32)
        lists[at + 5 : at + 8, :] = jnp.zeros((3, count), jnp.int32)
        inverses[i : i + 1, :] = table[4:5]


def bond_lists(offsets, slab, rows, halves, halo):
    count = offsets.shape[0]
    body = functools.partial(
        lists_kernel, slab=slab, rows=rows, halves=halves, slabs=lax.axis_size("pts"), halo=halo
    )
    device = lax.axis_index("pts").astype(jnp.int32).reshape(1)
    vmem = pl.BlockSpec(memory_space=pltpu.VMEM)
    lists, inverses = pl.pallas_call(
        body,
        out_shape=(
            jax.ShapeDtypeStruct((slab * ROWS_OF_LIST, count), jnp.int32),
            jax.ShapeDtypeStruct((slab, count), jnp.float32),
        ),
        in_specs=[pl.BlockSpec(memory_space=pltpu.SMEM), vmem],
        out_specs=(vmem, vmem),
        cost_estimate=pl.CostEstimate(flops=8_000_000, transcendentals=0, bytes_accessed=0),
        name="halo_lists" if halo else "own_lists",
    )(device, offsets.astype(jnp.int32).T)
    return lists.reshape(-1), inverses.reshape(-1)


def shifted(parts, c, lane):
    if c == 0:
        return parts
    turned = [pltpu.roll(part, (-c) % LANES, 1) for part in parts]
    result = []
    for h in range(len(parts)):
        other = h + 1 if c > 0 else h - 1
        if 0 <= other < len(parts):
            keep = lane < LANES - c if c > 0 else lane >= -c
            result.append(jnp.where(keep, turned[h], turned[other]))
        else:
            result.append(turned[h])
    return result


def bonds_kernel(lists, inverses, places, *refs, halo, slab, rows, halves, count, pieces, segments, seg_rows, started, started_at, keep, given):
    refs = list(refs)
    take = lambda n: [refs.pop(0) for _ in range(n)]
    own = take(pieces)
    lows = take(pieces) if halo and not given else []
    highs = take(pieces) if halo and not given else []
    kept = take(2) if given else None
    mask = refs.pop(0)
    init = refs.pop(0) if started else None
    out = refs.pop(0)
    copies, outside = kept or take(2)
    py, plain, buffer, sems = refs
    stride = rows + TILE
    width = own[0].shape[2]
    tiles = width // TILE
    low, high, total = copy_bases(slab, halo)
    middle = 0.5 * (slab - 1)
    lane = lax.broadcasted_iota(jnp.int32, (TILE, LANES), 1)
    row = lax.broadcasted_iota(jnp.int32, (TILE, LANES), 0)
    zero = jnp.zeros((TILE, LANES), jnp.float32)
    me = places[0]

    def first_row(s):
        if s == 0:
            return pl.multiple_of(me * width, TILE)
        below = me - s
        return pl.multiple_of(jnp.where(below < 0, below + pieces, below) * width, TILE)

    piece_row = [first_row(s) for s in range(pieces)]
    parts = sems.shape[1]
    each = count // parts
    items = len(segments) * slab

    def seg_row(g):
        row0 = piece_row[segments[0]]
        for n, s in enumerate(segments):
            row0 = jnp.where(g == n, piece_row[s], row0)
        return pl.multiple_of(row0, TILE)

    def fetch(t, slot):
        at = seg_row(t // slab)
        return [
            pltpu.make_async_copy(
                mask.at[pl.ds(n * each, each), t % slab, pl.ds(at, seg_rows), :],
                buffer.at[slot, pl.ds(n * each, each)],
                sems.at[slot, n],
            )
            for n in range(parts)
        ]

    for t in range(min(SLOTS - 1, items)):
        for copy in fetch(t, t):
            copy.start()

    def spread(piece, field, plane, x, first_row, places_of):
        along_x = jnp.where(field == 0, x, 0.0)
        along_z = jnp.where(field == 2, SPACING, 0.0)
        for tile in range(tiles):
            at = tile * TILE
            parts = [
                piece[field, plane, at : at + TILE, h * LANES : (h + 1) * LANES] + along_x
                for h in range(halves)
            ]
            for c, to in places_of:
                moved = shifted([part + along_z * float(c) if c else part for part in parts], c, lane)
                for h in range(halves):
                    put = (to * 4 + field) * (halves * stride) + (h * stride + TILE + at)
                    copies[pl.ds(pl.multiple_of(first_row + put, TILE), TILE), :] = moved[h]

    def one_field(field, carry):
        for s in range(pieces):
            if halo:
                for d in range(1, REACH + 1):
                    span = range(-cut(d), cut(d) + 1)
                    below = [(c, low[c + REACH] - d) for c in span]
                    above = [(c, high[c + REACH] + slab + d - 1) for c in span]
                    spread(lows[s], field, REACH - d, SPACING * (-d - middle), piece_row[s], below)
                    spread(highs[s], field, d - 1, SPACING * (slab + d - 1 - middle), piece_row[s], above)
            else:
                for i in range(slab):
                    to = [(c, low[c + REACH] + i) for c in range(-REACH, REACH + 1)]
                    spread(own[s], field, i, SPACING * (i - middle), piece_row[s], to)
        return carry

    if not given:
        def clear(n, carry):
            copies[pl.ds(pl.multiple_of(n * stride, TILE), TILE), :] = zero
            return carry

        lax.fori_loop(0, total * 4 * halves, clear, 0, unroll=16)
        copies[total * 4 * halves * stride : total * 4 * halves * stride + TILE, :] = zero

        lax.fori_loop(0, 4, one_field, 0)

        for c in range(-REACH, REACH + 1):
            for h in range(halves):
                z = lane + (h * LANES + c)
                z_out = (z < 0) | (z >= halves * LANES)
                for tile in range(-1, rows // TILE + 1):
                    r = row + tile * TILE
                    gone = z_out | (r < 0) | (r >= rows)
                    at = ((c + REACH) * halves + h) * (rows + 2 * TILE) + (tile + 1) * TILE
                    outside[at : at + TILE, :] = gone.astype(jnp.int32)

    for g, s in enumerate(segments):

        def one_tile(n, carry, s=s, g=g):
            plane = n // (seg_rows // TILE)
            at = n % (seg_rows // TILE) * TILE
            source = pl.ds(pl.multiple_of(at, TILE), TILE)
            x = SPACING * (plane.astype(jnp.float32) - middle)
            for h in range(halves):
                lanes = slice(h * LANES, (h + 1) * LANES)
                to = (plane * halves + h) * rows + g * seg_rows + at
                here = pl.ds(pl.multiple_of(to, TILE), TILE)
                plain[0, here, :] = own[s][0, plane, source, lanes] + x
                plain[1, here, :] = own[s][2, plane, source, lanes]
                plain[2, here, :] = own[s][3, plane, source, lanes]
                uy = own[s][1, plane, source, lanes]
                for n in range(SHIFTS):
                    there = pl.ds(pl.multiple_of(to + n * (slab * halves * rows), TILE), TILE)
                    py[there, :] = uy - SPACING * (n - REACH)
            return carry

        lax.fori_loop(0, slab * (seg_rows // TILE), one_tile, 0, unroll=2)

    short = math.gcd(count, SHORT)
    unit = math.gcd(seg_rows, UNIT)

    def one_item(t, carry):
        slot = lax.rem(t, SLOTS)
        for copy in fetch(t, slot):
            copy.wait()

        @pl.when(t + SLOTS - 1 < items)
        def _():
            for copy in fetch(t + SLOTS - 1, lax.rem(t + SLOTS - 1, SLOTS)):
                copy.start()

        g, i = t // slab, t % slab
        row0 = seg_row(g)
        table = i * (ROWS_OF_LIST * count)
        bonds = lists[table + 4 * count]
        whole = bonds // LONG

        def one_unit(n, carry):
            local = g * seg_rows + n * unit
            here = row0 + n * unit
            grid = [(r, h) for r in range(0, unit, TILE) for h in range(halves)]
            first_p = (i * halves) * rows + local
            mine = [
                [plain[f, pl.ds(pl.multiple_of(first_p + h * rows + r, TILE), TILE), :] for f in range(3)]
                for r, h in grid
            ]
            mask_row = pl.multiple_of(n * unit, TILE)

            def step(first, number, totals):
                totals = list(totals)
                for u in range(number):
                    e = table + first + u
                    q = lists[e] + here
                    o = lists[e + count] + here
                    ay = lists[e + 2 * count] + local
                    k = lists[e + 3 * count]
                    inverse = inverses[i * count + first + u]
                    for n, (r, h) in enumerate(grid):
                        own_x, own_z, own_k = mine[n]

                        def near(field):
                            return copies[pl.ds(q + ((field * halves + h) * stride + r), TILE), :]

                        rx = near(0) - own_x
                        ry = near(1) - py[pl.ds(pl.multiple_of(ay + (h * rows + r), TILE), TILE), :]
                        rz = near(2) - own_z
                        inv = lax.rsqrt(rx * rx + ry * ry + rz * rz)
                        gone = outside[pl.ds(o + (h * (rows + 2 * TILE) + r), TILE), :]
                        alive = buffer[slot, k, pl.ds(mask_row + r, TILE), h * LANES : (h + 1) * LANES]
                        factor = jnp.where(alive > gone, inverse, 0.0)
                        w = (inverse - inv) * (near(3) + own_k) * factor
                        totals[3 * n] += w * rx
                        totals[3 * n + 1] += w * ry
                        totals[3 * n + 2] += w * rz
                return tuple(totals)

            totals = (zero,) * (3 * len(grid))
            totals = lax.fori_loop(0, whole, lambda m, x: step(m * LONG, LONG, x), totals)
            rest = (bonds - whole * LONG + short - 1) // short
            totals = lax.fori_loop(
                0, rest, lambda m, x: step(whole * LONG + m * short, short, x), totals
            )
            for n, (r, h) in enumerate(grid):
                lanes = slice(h * LANES, (h + 1) * LANES)
                for f in range(3):
                    value = totals[3 * n + f]
                    if started:
                        value = value + init[g + started_at, f, i, pl.ds(mask_row + r, TILE), lanes]
                    out[g, f, i, pl.ds(mask_row + r, TILE), lanes] = value
            return carry

        lax.fori_loop(0, seg_rows // unit, one_unit, 0)
        return carry

    lax.fori_loop(0, items, one_item, 0)


def bonds(lists, places, pieces, sides, intact, segments, seg_rows, rows, init, started_at, name, share, keep=False, given=None):
    count, slab, _, depth = intact.shape
    halves = depth // LANES
    halo = sides is not None
    _, _, total = copy_bases(slab, halo)
    blocks = list(pieces)
    if given is not None:
        blocks += list(given)
    elif halo:
        blocks += list(sides[0]) + list(sides[1])
    vmem, smem = pl.BlockSpec(memory_space=pltpu.VMEM), pl.BlockSpec(memory_space=pltpu.SMEM)
    started = init is not None
    body = functools.partial(
        bonds_kernel,
        halo=halo,
        slab=slab,
        rows=rows,
        halves=halves,
        count=count,
        pieces=len(pieces),
        segments=segments,
        seg_rows=seg_rows,
        started=started,
        started_at=started_at,
        keep=keep,
        given=given is not None,
    )
    sums = jax.ShapeDtypeStruct((len(segments), 3, slab, seg_rows, depth), jnp.float32)
    tables = [
        pltpu.VMEM((total * 4 * halves * (rows + TILE) + TILE, LANES), jnp.float32),
        pltpu.VMEM((SHIFTS * halves * (rows + 2 * TILE), LANES), jnp.int32),
    ]
    table = pltpu.VMEM((SHIFTS * slab * halves * rows, LANES), jnp.float32)
    plain = pltpu.VMEM((3, slab * halves * rows, LANES), jnp.float32)
    return pl.pallas_call(
        body,
        out_shape=[sums, *tables] if keep else sums,
        in_specs=[smem] * 3
        + [vmem] * len(blocks)
        + [pl.BlockSpec(memory_space=pl.ANY)]
        + [vmem] * started,
        out_specs=[vmem] * 3 if keep else vmem,
        scratch_shapes=([] if keep or given is not None else tables)
        + [
            table,
            plain,
            pltpu.VMEM((SLOTS, count, seg_rows, depth), jnp.int32),
            pltpu.SemaphoreType.DMA((SLOTS, math.gcd(count, PARTS))),
        ],
        compiler_params=pltpu.CompilerParams(vmem_limit_bytes=LIMIT),
        cost_estimate=pl.CostEstimate(
            flops=int(40 * share * count * slab * rows * depth), transcendentals=0, bytes_accessed=intact.size * 4
        ),
        name=name,
    )(*lists, places, *blocks, intact, *([init] if started else []))


def on_device(displacement, velocity, stiffness, offsets, intact):
    slab, width, depth = stiffness.shape
    rows = intact.shape[2]
    halves = depth // LANES
    number = lax.axis_size("bond")
    me = lax.axis_index("bond")
    count = lax.axis_size("pts")
    forward = [(i, i + 1) for i in range(count - 1)]
    backward = [(t, s) for s, t in forward]

    pieces = [jnp.concatenate([displacement, stiffness[None]], axis=0)]
    for s in range(1, number):
        pieces.append(lax.ppermute(pieces[0], "bond", [(j, (j + s) % number) for j in range(number)]))
    own_lists = bond_lists(offsets, slab, rows, halves, False)
    halo_lists = bond_lists(offsets, slab, rows, halves, True)
    received, own_lists, halo_lists = lax.optimization_barrier((pieces[1:], own_lists, halo_lists))
    pieces = pieces[:1] + list(received)
    lows = [lax.ppermute(x[:, slab - REACH :], "pts", forward) for x in pieces]
    highs = [lax.ppermute(x[:, :REACH], "pts", backward) for x in pieces]
    place = me.astype(jnp.int32).reshape(1)
    every = list(range(number))
    inner = bonds(
        own_lists, place, pieces, None, intact, every, width, rows, None, 0, "own_planes", 0.64
    )
    sides = (lows, highs)
    theirs, *kept = bonds(
        halo_lists, place, pieces, sides, intact, every[1:], width, rows, inner, 1,
        "their_rows", 0.36 * (number - 1) / number, keep=True,
    )
    back = [
        lax.ppermute(theirs[s - 1], "bond", [(j, (j - s) % number) for j in range(number)])
        for s in range(1, number)
    ]
    ours = bonds(
        halo_lists, place, pieces, sides, intact, every[:1], width, rows, inner, 0,
        "our_rows", 0.36 / number, given=kept,
    )
    total = ours[0]
    for part in back:
        total = total + part
    new_velocity = velocity + (0.5 * FORCE_SCALE * TIME_STEP) * total
    new_displacement = displacement + TIME_STEP * new_velocity
    return (new_displacement, new_velocity)


def solution(mesh):
    return jax.shard_map(
        on_device,
        mesh=mesh,
        in_specs=(
            P(None, "pts", "bond", None),
            P(None, "pts", "bond", None),
            P("pts", "bond", None),
            P("bond", None),
            P("bond", "pts", None, None),
        ),
        out_specs=(P(None, "pts", "bond", None), P(None, "pts", "bond", None)),
        check_vma=False,
    )
```

```python
import functools
import math

import jax
import jax.numpy as jnp
from jax import lax
from jax.experimental import pallas as pl
from jax.experimental.pallas import tpu as pltpu
from jax.sharding import PartitionSpec as P

REACH = 4
SPACING = 6.0
FORCE_SCALE = 8.0
TIME_STEP = 0.5
LANES = 128
TILE = 8
UNIT = 16
LONG = 8
SHORT = 2
SLOTS = 6
PARTS = 2
LIMIT = 28 * 1024 * 1024
SHIFTS = 2 * REACH + 1


def cut(d):
    return math.isqrt(REACH * REACH - d * d)


def copy_bases(slab, halo):
    low, high, total = [], [], 0
    for c in range(-REACH, REACH + 1):
        if halo:
            low.append(total + cut(c))
            high.append(total + cut(c) - slab)
            total += 2 * cut(c)
        else:
            low.append(total)
            high.append(total)
            total += slab
    return low, high, total


ROWS_OF_LIST = 8


def lists_kernel(device, shift, *outs, slab, rows, halves, slabs):
    stride = rows + TILE
    a, b, c = [shift[n : n + 1, :] for n in range(3)]
    count = shift.shape[1]
    first = device[0] * slab
    inverse = 1.0 / (SPACING * jnp.sqrt((a * a + b * b + c * c).astype(jnp.float32)))
    bond = lax.broadcasted_iota(jnp.int32, (1, count), 1)
    down = lax.broadcasted_iota(jnp.int32, (count, count), 0)
    across = lax.broadcasted_iota(jnp.int32, (count, count), 1)
    earlier = (down < across).astype(jnp.float32)
    for halo, lists, inverses in ((False, *outs[:2]), (True, *outs[2:])):
        low, high, _ = copy_bases(slab, halo)
        for i in range(slab):
            plane = a + i
            inside = (plane >= 0) & (plane < slab)
            if halo:
                whole = plane + first
                member = (~inside) & (whole >= 0) & (whole < slab * slabs)
            else:
                member = inside
            base = jnp.zeros_like(plane)
            for n in range(SHIFTS):
                base = jnp.where(c == n - REACH, jnp.where(plane < 0, low[n], high[n]), base)
            ones = jnp.where(member, 1.0, 0.0)
            place = jnp.dot(jnp.broadcast_to(ones, (8, count)), earlier, precision=lax.Precision.HIGHEST)[0:1]
            spot = (place.astype(jnp.int32) == down) & (jnp.broadcast_to(ones, (count, count)) > 0.5)
            values = [
                (base + plane) * (4 * halves * stride) + TILE + b,
                (c + REACH) * (halves * (rows + 2 * TILE)) + TILE + b,
                ((b + REACH) * slab + i) * (halves * rows),
                bond,
            ]
            values = [v.astype(jnp.float32) for v in values] + [inverse] + [jnp.zeros_like(inverse)] * 3
            table = lax.dot_general(
                jnp.concatenate(values, axis=0),
                jnp.where(spot, 1.0, 0.0),
                (((1,), (1,)), ((), ())),
                precision=lax.Precision.HIGHEST,
                preferred_element_type=jnp.float32,
            )
            number = jnp.broadcast_to(jnp.sum(ones, axis=1, keepdims=True), (1, count))
            at = i * ROWS_OF_LIST
            lists[at : at + 4, :] = (table[0:4] + 0.5).astype(jnp.int32)
            lists[at + 4 : at + 5, :] = number.astype(jnp.int32)
            lists[at + 5 : at + 8, :] = jnp.zeros((3, count), jnp.int32)
            inverses[i : i + 1, :] = table[4:5]


def bond_lists(offsets, slab, rows, halves):
    count = offsets.shape[0]
    body = functools.partial(
        lists_kernel, slab=slab, rows=rows, halves=halves, slabs=lax.axis_size("pts")
    )
    device = lax.axis_index("pts").astype(jnp.int32).reshape(1)
    vmem = pl.BlockSpec(memory_space=pltpu.VMEM)
    results = pl.pallas_call(
        body,
        out_shape=[
            pltpu.VMEM((slab * ROWS_OF_LIST, count), jnp.int32),
            pltpu.VMEM((slab, count), jnp.float32),
        ]
        * 2,
        in_specs=[pl.BlockSpec(memory_space=pltpu.SMEM), vmem],
        out_specs=[vmem] * 4,
        cost_estimate=pl.CostEstimate(flops=16_000_000, transcendentals=0, bytes_accessed=0),
        name="lists",
    )(device, offsets.astype(jnp.int32).T)
    flat = [x.reshape(-1) for x in results]
    return flat[:2], flat[2:]


def shifted(parts, c, lane):
    if c == 0:
        return parts
    turned = [pltpu.roll(part, (-c) % LANES, 1) for part in parts]
    result = []
    for h in range(len(parts)):
        other = h + 1 if c > 0 else h - 1
        if 0 <= other < len(parts):
            keep = lane < LANES - c if c > 0 else lane >= -c
            result.append(jnp.where(keep, turned[h], turned[other]))
        else:
            result.append(turned[h])
    return result


def bonds_kernel(lists, inverses, places, *refs, halo, slab, rows, halves, count, pieces, segments, seg_rows, started, started_at, keep, given):
    refs = list(refs)
    take = lambda n: [refs.pop(0) for _ in range(n)]
    own = take(pieces)
    lows = take(pieces) if halo and not given else []
    highs = take(pieces) if halo and not given else []
    kept = take(2) if given else None
    mask = refs.pop(0)
    init = refs.pop(0) if started else None
    out = refs.pop(0)
    copies, outside = kept or take(2)
    py, plain, buffer, sems = refs
    stride = rows + TILE
    width = own[0].shape[2]
    tiles = width // TILE
    low, high, total = copy_bases(slab, halo)
    middle = 0.5 * (slab - 1)
    lane = lax.broadcasted_iota(jnp.int32, (TILE, LANES), 1)
    row = lax.broadcasted_iota(jnp.int32, (TILE, LANES), 0)
    zero = jnp.zeros((TILE, LANES), jnp.float32)
    me = places[0]

    def first_row(s):
        if s == 0:
            return pl.multiple_of(me * width, TILE)
        below = me - s
        return pl.multiple_of(jnp.where(below < 0, below + pieces, below) * width, TILE)

    piece_row = [first_row(s) for s in range(pieces)]
    parts = sems.shape[1]
    each = count // parts
    unit = math.gcd(seg_rows, UNIT)
    units = seg_rows // unit
    items = len(segments) * slab * units

    def seg_row(g):
        row0 = piece_row[segments[0]]
        for n, s in enumerate(segments):
            row0 = jnp.where(g == n, piece_row[s], row0)
        return pl.multiple_of(row0, TILE)

    def fetch(t, slot):
        at = pl.multiple_of(seg_row(t // (slab * units)) + t % units * unit, TILE)
        return [
            pltpu.make_async_copy(
                mask.at[pl.ds(n * each, each), t // units % slab, pl.ds(at, unit), :],
                buffer.at[slot, pl.ds(n * each, each)],
                sems.at[slot, n],
            )
            for n in range(parts)
        ]

    for t in range(min(SLOTS - 1, items)):
        for copy in fetch(t, t):
            copy.start()

    def spread(piece, field, plane, x, first_row, places_of):
        along_x = jnp.where(field == 0, x, 0.0)
        along_z = jnp.where(field == 2, SPACING, 0.0)
        for tile in range(tiles):
            at = tile * TILE
            parts = [
                piece[field, plane, at : at + TILE, h * LANES : (h + 1) * LANES] + along_x
                for h in range(halves)
            ]
            for c, to in places_of:
                moved = shifted([part + along_z * float(c) if c else part for part in parts], c, lane)
                for h in range(halves):
                    put = (to * 4 + field) * (halves * stride) + (h * stride + TILE + at)
                    copies[pl.ds(pl.multiple_of(first_row + put, TILE), TILE), :] = moved[h]

    def one_field(field, carry):
        for s in range(pieces):
            if halo:
                for d in range(1, REACH + 1):
                    span = range(-cut(d), cut(d) + 1)
                    below = [(c, low[c + REACH] - d) for c in span]
                    above = [(c, high[c + REACH] + slab + d - 1) for c in span]
                    spread(lows[s], field, REACH - d, SPACING * (-d - middle), piece_row[s], below)
                    spread(highs[s], field, d - 1, SPACING * (slab + d - 1 - middle), piece_row[s], above)
            else:
                for i in range(slab):
                    to = [(c, low[c + REACH] + i) for c in range(-REACH, REACH + 1)]
                    spread(own[s], field, i, SPACING * (i - middle), piece_row[s], to)
        return carry

    if not given:
        def clear(n, carry):
            copies[pl.ds(pl.multiple_of(n * stride, TILE), TILE), :] = zero
            return carry

        lax.fori_loop(0, total * 4 * halves, clear, 0, unroll=16)
        copies[total * 4 * halves * stride : total * 4 * halves * stride + TILE, :] = zero

        lax.fori_loop(0, 4, one_field, 0)

        for c in range(-REACH, REACH + 1):
            for h in range(halves):
                z = lane + (h * LANES + c)
                z_out = (z < 0) | (z >= halves * LANES)
                for tile in range(-1, rows // TILE + 1):
                    r = row + tile * TILE
                    gone = z_out | (r < 0) | (r >= rows)
                    at = ((c + REACH) * halves + h) * (rows + 2 * TILE) + (tile + 1) * TILE
                    outside[at : at + TILE, :] = gone.astype(jnp.int32)

    for g, s in enumerate(segments):

        def one_tile(n, carry, s=s, g=g):
            plane = n // (seg_rows // TILE)
            at = n % (seg_rows // TILE) * TILE
            source = pl.ds(pl.multiple_of(at, TILE), TILE)
            x = SPACING * (plane.astype(jnp.float32) - middle)
            for h in range(halves):
                lanes = slice(h * LANES, (h + 1) * LANES)
                to = (plane * halves + h) * rows + g * seg_rows + at
                here = pl.ds(pl.multiple_of(to, TILE), TILE)
                plain[0, here, :] = own[s][0, plane, source, lanes] + x
                plain[1, here, :] = own[s][2, plane, source, lanes]
                plain[2, here, :] = own[s][3, plane, source, lanes]
                uy = own[s][1, plane, source, lanes]
                for n in range(SHIFTS):
                    there = pl.ds(pl.multiple_of(to + n * (slab * halves * rows), TILE), TILE)
                    py[there, :] = uy - SPACING * (n - REACH)
            return carry

        lax.fori_loop(0, slab * (seg_rows // TILE), one_tile, 0, unroll=2)

    short = math.gcd(count, SHORT)
    def one_item(t, carry):
        slot = lax.rem(t, SLOTS)
        for copy in fetch(t, slot):
            copy.wait()

        @pl.when(t + SLOTS - 1 < items)
        def _():
            for copy in fetch(t + SLOTS - 1, lax.rem(t + SLOTS - 1, SLOTS)):
                copy.start()

        g, i, n = t // (slab * units), t // units % slab, t % units
        row0 = seg_row(g)
        table = i * (ROWS_OF_LIST * count)
        bonds = lists[table + 4 * count]
        whole = bonds // LONG

        local = g * seg_rows + n * unit
        here = row0 + n * unit
        grid = [(r, h) for r in range(0, unit, TILE) for h in range(halves)]
        first_p = (i * halves) * rows + local
        mine = [
            [plain[f, pl.ds(pl.multiple_of(first_p + h * rows + r, TILE), TILE), :] for f in range(3)]
            for r, h in grid
        ]
        mask_row = pl.multiple_of(n * unit, TILE)

        def step(first, number, totals):
            totals = list(totals)
            for u in range(number):
                e = table + first + u
                q = lists[e] + here
                o = lists[e + count] + here
                ay = lists[e + 2 * count] + local
                k = lists[e + 3 * count]
                inverse = inverses[i * count + first + u]
                for m, (r, h) in enumerate(grid):
                    own_x, own_z, own_k = mine[m]

                    def near(field):
                        return copies[pl.ds(q + ((field * halves + h) * stride + r), TILE), :]

                    rx = near(0) - own_x
                    ry = near(1) - py[pl.ds(pl.multiple_of(ay + (h * rows + r), TILE), TILE), :]
                    rz = near(2) - own_z
                    inv = lax.rsqrt(rx * rx + ry * ry + rz * rz)
                    gone = outside[pl.ds(o + (h * (rows + 2 * TILE) + r), TILE), :]
                    alive = buffer[slot, k, r : r + TILE, h * LANES : (h + 1) * LANES]
                    factor = jnp.where(alive > gone, inverse, 0.0)
                    w = (inverse - inv) * (near(3) + own_k) * factor
                    totals[3 * m] += w * rx
                    totals[3 * m + 1] += w * ry
                    totals[3 * m + 2] += w * rz
            return tuple(totals)

        totals = (zero,) * (3 * len(grid))
        totals = lax.fori_loop(0, whole, lambda j, x: step(j * LONG, LONG, x), totals)
        rest = (bonds - whole * LONG + short - 1) // short
        totals = lax.fori_loop(
            0, rest, lambda j, x: step(whole * LONG + j * short, short, x), totals
        )
        for m, (r, h) in enumerate(grid):
            lanes = slice(h * LANES, (h + 1) * LANES)
            for f in range(3):
                value = totals[3 * m + f]
                if started:
                    value = value + init[g + started_at, f, i, pl.ds(mask_row + r, TILE), lanes]
                out[g, f, i, pl.ds(mask_row + r, TILE), lanes] = value
        return carry

    lax.fori_loop(0, items, one_item, 0)


def bonds(lists, places, pieces, sides, intact, segments, seg_rows, rows, init, started_at, name, share, keep=False, given=None):
    count, slab, _, depth = intact.shape
    halves = depth // LANES
    halo = sides is not None
    _, _, total = copy_bases(slab, halo)
    blocks = list(pieces)
    if given is not None:
        blocks += list(given)
    elif halo:
        blocks += list(sides[0]) + list(sides[1])
    vmem, smem = pl.BlockSpec(memory_space=pltpu.VMEM), pl.BlockSpec(memory_space=pltpu.SMEM)
    started = init is not None
    body = functools.partial(
        bonds_kernel,
        halo=halo,
        slab=slab,
        rows=rows,
        halves=halves,
        count=count,
        pieces=len(pieces),
        segments=segments,
        seg_rows=seg_rows,
        started=started,
        started_at=started_at,
        keep=keep,
        given=given is not None,
    )
    sums = jax.ShapeDtypeStruct((len(segments), 3, slab, seg_rows, depth), jnp.float32)
    tables = [
        pltpu.VMEM((total * 4 * halves * (rows + TILE) + TILE, LANES), jnp.float32),
        pltpu.VMEM((SHIFTS * halves * (rows + 2 * TILE), LANES), jnp.int32),
    ]
    table = pltpu.VMEM((SHIFTS * slab * halves * rows, LANES), jnp.float32)
    plain = pltpu.VMEM((3, slab * halves * rows, LANES), jnp.float32)
    return pl.pallas_call(
        body,
        out_shape=[sums, *tables] if keep else sums,
        in_specs=[smem] * 3
        + [vmem] * len(blocks)
        + [pl.BlockSpec(memory_space=pl.ANY)]
        + [vmem] * started,
        out_specs=[vmem] * 3 if keep else vmem,
        scratch_shapes=([] if keep or given is not None else tables)
        + [
            table,
            plain,
            pltpu.VMEM((SLOTS, count, math.gcd(seg_rows, UNIT), depth), jnp.int32),
            pltpu.SemaphoreType.DMA((SLOTS, math.gcd(count, PARTS))),
        ],
        compiler_params=pltpu.CompilerParams(vmem_limit_bytes=LIMIT),
        cost_estimate=pl.CostEstimate(
            flops=int(40 * share * count * slab * rows * depth), transcendentals=0, bytes_accessed=intact.size * 4
        ),
        name=name,
    )(*lists, places, *blocks, intact, *([init] if started else []))


def on_device(displacement, velocity, stiffness, offsets, intact):
    slab, width, depth = stiffness.shape
    rows = intact.shape[2]
    halves = depth // LANES
    number = lax.axis_size("bond")
    me = lax.axis_index("bond")
    count = lax.axis_size("pts")
    forward = [(i, i + 1) for i in range(count - 1)]
    backward = [(t, s) for s, t in forward]

    pieces = [jnp.concatenate([displacement, stiffness[None]], axis=0)]
    for s in range(1, number):
        pieces.append(lax.ppermute(pieces[0], "bond", [(j, (j + s) % number) for j in range(number)]))
    own_lists, halo_lists = bond_lists(offsets, slab, rows, halves)
    received, own_lists, halo_lists = lax.optimization_barrier((pieces[1:], own_lists, halo_lists))
    pieces = pieces[:1] + list(received)
    lows = [lax.ppermute(x[:, slab - REACH :], "pts", forward) for x in pieces]
    highs = [lax.ppermute(x[:, :REACH], "pts", backward) for x in pieces]
    place = me.astype(jnp.int32).reshape(1)
    every = list(range(number))
    inner = bonds(
        own_lists, place, pieces, None, intact, every, width, rows, None, 0, "own_planes", 0.64
    )
    sides = (lows, highs)
    theirs, *kept = bonds(
        halo_lists, place, pieces, sides, intact, every[1:], width, rows, inner, 1,
        "their_rows", 0.36 * (number - 1) / number, keep=True,
    )
    back = [
        lax.ppermute(theirs[s - 1], "bond", [(j, (j - s) % number) for j in range(number)])
        for s in range(1, number)
    ]
    ours = bonds(
        halo_lists, place, pieces, sides, intact, every[:1], width, rows, inner, 0,
        "our_rows", 0.36 / number, given=kept,
    )
    total = ours[0]
    for part in back:
        total = total + part
    new_velocity = velocity + (0.5 * FORCE_SCALE * TIME_STEP) * total
    new_displacement = displacement + TIME_STEP * new_velocity
    return (new_displacement, new_velocity)


def solution(mesh):
    return jax.shard_map(
        on_device,
        mesh=mesh,
        in_specs=(
            P(None, "pts", "bond", None),
            P(None, "pts", "bond", None),
            P("pts", "bond", None),
            P("bond", None),
            P("bond", "pts", None, None),
        ),
        out_specs=(P(None, "pts", "bond", None), P(None, "pts", "bond", None)),
        check_vma=False,
    )
```
